256 devices in a mesh: grp: 2 (over z), row: 16 (over x, core), col: 8 (over y).
Axes of the slice: x: 8, y: 8, z: 2, core: 2. Of those that a mesh axis runs over, the one named last changes fastest.
The devices are a block of a 8x8x16 slice.
Arguments:
- perturbation: bfloat16 [4, 12000, 12000], P('grp', 'row', 'col'), parts along dimension 0, may hold values from -96 to 96
- occ_coeffs: bfloat16 [12000, 2000], P('row', 'col'), may hold values from -0.0546875 to 0.0546875
- vir_coeffs: bfloat16 [12000, 512], P('col', 'row'), may hold values from -0.0546875 to 0.0546875
- occ_energies: float32 [2000], replicated, may hold values from -1 to -0.1
- vir_energies: float32 [512], replicated, may hold values from 0.1 to 1.5
Outputs:
- density_response: bfloat16 [4, 12000, 12000], P('grp', 'row', 'col'), parts along dimension 0
The draws below stay inside these ranges and needn't reach their ends.
There are 2 independent parts, one for each index of `grp`. The reference program is written for one: setup_inputs(seed, part) draws one part's arguments, and reference() takes and returns one part's arrays. A program takes and returns all parts, laid end to end along the dimension named above; an argument that names none is the same for every part. Nothing has to cross between parts.
All inputs are finite; a program needn't handle non-finite values.
Results may differ from the reference program's by a relative error of at most 0.0098.
Values may be sent and summed in bfloat16 or wider, within the bound.
A program may use at most 64 MiB of HBM per device.

```python
import jax
import jax.numpy as jnp
from jax import lax

NB = 12000
NOCC = 2000
NV = 512
PERT = 2


def block_levels(rng, shape, cuts, smallest, high):
    factor_of = 1.0
    for dim, shards_of in cuts:
        draws = jax.random.uniform(jax.random.fold_in(jax.random.fold_in(rng, 6), dim), (shards_of,), jnp.float32, smallest / len(cuts), high / len(cuts))
        factor_of = factor_of * jnp.repeat(jnp.exp(draws), shape[dim] // shards_of).reshape((-1,) + (1,) * (len(shape) - 1 - dim))
    return factor_of


def scatter_about(key, shape, spread, bound, cuts=(), held_as=jnp.bfloat16):
    array = spread * jax.random.normal(key, shape, jnp.float32)
    if cuts:
        array = array * block_levels(key, shape, cuts, -0.22, 0.18)
    return jnp.clip(array, -bound, bound).astype(held_as)


def setup_inputs(seed: int = 0, part: int = 0) -> dict:
    seeds = jax.random.split(jax.random.key(seed), 6)
    part_keys = jax.random.split(jax.random.fold_in(seeds[5], part), 6)
    return {
        "perturbation": scatter_about(part_keys[0], (PERT, NB, NB), 16.0, 96.0, ((1, 16), (2, 8))),
        "occ_coeffs": scatter_about(seeds[1], (NB, NOCC), NB ** -0.5, 0.0546875, ((0, 16), (1, 8))),
        "vir_coeffs": scatter_about(seeds[2], (NB, NV), NB ** -0.5, 0.0546875, ((0, 8), (1, 16))),
        "occ_energies": jnp.clip(jax.random.uniform(seeds[3], (NOCC,), jnp.float32, -1.0, -0.1), -1.0, -0.1),
        "vir_energies": jnp.clip(jax.random.uniform(seeds[4], (NV,), jnp.float32, 0.1, 1.5), 0.1, 1.5),
    }


def reference(perturbation, occ_coeffs, vir_coeffs, occ_energies, vir_energies):
    gaps = occ_energies[:, None] - vir_energies[None, :]
    occ_wide = occ_coeffs.astype(jnp.float32)
    results = []
    for index in range(PERT):
        image = jnp.dot(perturbation[index], vir_coeffs, preferred_element_type=jnp.float32)
        coupling = jnp.dot(occ_wide.T, image, precision=lax.Precision.HIGHEST)
        response = (coupling / gaps).astype(jnp.bfloat16)
        mixed = jnp.dot(occ_coeffs, response, preferred_element_type=jnp.float32).astype(jnp.bfloat16)
        results.append(jnp.dot(mixed, vir_coeffs.T, preferred_element_type=jnp.float32).astype(jnp.bfloat16))
    return jnp.stack(results)
```

```python
import functools

import jax
import jax.numpy as jnp
from jax import lax
from jax.experimental import pallas as pl
from jax.experimental.pallas import tpu as pltpu
from jax.sharding import PartitionSpec as P

MESH = pl.DeviceIdType.MESH
BF16, F32 = jnp.bfloat16, jnp.float32
LANES = 128
NT = (((1,), (1,)), ((), ()))


def round_up(n, m):
    return -(-n // m) * m


def exchange_kernel(dims, *refs):
    nrow, ncol, rows, cols, occ, vir = dims
    (h_hbm, vt_ref, c_ref, eo_ref, ev_ref, mix_ref, vtall_ref) = refs[:7]
    (hbuf, xs, xo, cbuf, rs0, rsb, ct, cx, red, xr, rb, eo_pad) = refs[7:19]
    (h_sem, v_s, v_r, vd_s, vd_r, c_s, c_r, r_s, r_r) = refs[19:28]
    (d_s, d_r, a_s, a_r, g_s, g_r, e_s, e_r, m_s, m_r) = refs[28:]

    nx = nrow // 2
    half = ncol // 2
    hx = nx // 2
    mine = vt_ref.shape[0]
    padded = cbuf.shape[1]
    cut = rs0.shape[2]
    chunks = ((0, cut), (cut, padded - cut))

    r = lax.axis_index("row")
    y = lax.axis_index("col")
    x = lax.div(r, 2)
    k = lax.rem(r, 2)

    def at_y(m):
        return lax.rem(y + m + ncol, ncol)

    def at_x(m):
        return lax.rem(x + m + nx, nx)

    up, down = {"col": at_y(1)}, {"col": at_y(-1)}
    y_next = (up, down)
    x_next = ({"row": 2 * at_x(1) + k}, {"row": 2 * at_x(-1) + k})
    partner = {"row": 2 * x + 1 - k}

    def remote(src, dst, ss, rr, dev):
        return pltpu.make_async_remote_copy(
            src_ref=src, dst_ref=dst, send_sem=ss, recv_sem=rr, device_id=dev, device_id_type=MESH
        )

    h_copy = pltpu.make_async_copy(h_hbm, hbuf, h_sem)
    h_copy.start()

    barrier = pltpu.get_barrier_semaphore()
    for dev in y_next:
        pl.semaphore_signal(barrier, inc=1, device_id=dev, device_id_type=MESH)
    for j in range(1, nrow):
        pl.semaphore_signal(
            barrier, inc=1, device_id={"row": lax.rem(r + j, nrow)}, device_id_type=MESH
        )

    nocc = c_ref.shape[1]
    wide = cbuf.shape[2]
    cbuf[y, :, pl.ds(wide - LANES, LANES)] = jnp.zeros((padded, LANES), BF16)
    cbuf[y, pl.ds(padded - 16, 16), :] = jnp.zeros((16, wide), BF16)
    cbuf[y, pl.ds(0, rows), pl.ds(0, nocc)] = c_ref[...]
    vtall_ref[pl.ds(pl.multiple_of(r * mine, mine), mine), :] = vt_ref[...]

    eo_pad[...] = jnp.full(eo_pad.shape, -1.0, F32)
    eo_pad[:, pl.ds(0, occ)] = eo_ref[...]
    first = x * nocc + k * LANES
    near = pl.multiple_of(lax.div(first, LANES) * LANES, LANES)
    window = eo_pad[:, pl.ds(near, 2 * LANES)]
    window = pltpu.roll(
        jnp.broadcast_to(window, (8, 2 * LANES)), 2 * LANES - lax.rem(first, LANES), 1
    )
    eo = jnp.broadcast_to(window[0:1, 0:LANES], (LANES, LANES))
    ev = ev_ref[:, pl.ds(pl.multiple_of(lax.div(y, 2) * LANES, LANES), LANES)]
    ev = jnp.broadcast_to(ev, (LANES, LANES)).T
    gap = eo - ev

    pl.semaphore_wait(barrier, nrow + 1)

    def ring(buf, ss, rr):
        def copy(d, s, c, back):
            m = (s - 1) + back
            origin = at_y(-m) if d == 0 else at_y(m)
            n = 2 * (s - 1) + (c if s < half else 0)
            part = buf.at[origin, pl.ds(chunks[c][0], chunks[c][1])]
            return remote(part, part, ss.at[d, n], rr.at[d, n], y_next[d])

        def send(d, s, c):
            copy(d, s, c, 0).start()

        def arrived(d, s, c):
            copy(d, s, c, 1).wait_recv()

        def drain():
            for d in range(2):
                for s in range(1, half + 1):
                    for c in range(2) if s < half else (d,):
                        copy(d, s, c, 0).wait_send()

        return send, arrived, drain

    c_send, c_arrived, c_drain = ring(cbuf, c_s, c_r)
    for c in range(2):
        for d in range(2):
            c_send(d, 1, c)

    hm = mine // 2

    def v_copy(d, s, c, back):
        m = (s - 1) + back
        origin = at_x(-m) if d == 0 else at_x(m)
        n = 2 * (s - 1) + (c if s < hx else 0)
        start = pl.multiple_of((2 * origin + k) * mine + c * hm, hm)
        part = vtall_ref.at[pl.ds(start, hm)]
        return remote(part, part, v_s.at[d, n], v_r.at[d, n], x_next[d])

    def v_over(n, m, other):
        kk = 1 - k if other else k
        start = pl.multiple_of((2 * at_x(m) + kk) * mine, mine)
        part = vtall_ref.at[pl.ds(start, mine)]
        return remote(part, part, vd_s.at[n], vd_r.at[n], partner)

    for c in range(2):
        for d in range(2):
            v_copy(d, 1, c, 0).start()
    v_over(0, 0, False).start()
    over = [(0, 0)]

    def c_forward(s, c):
        for d in range(2):
            c_arrived(d, s, c)
            if s + 1 < half or c == d:
                c_send(d, s + 1, c)

    for s in range(1, hx):
        for c in range(2):
            for d in range(2):
                v_copy(d, s, c, 1).wait_recv()
                if s + 1 < hx or c == d:
                    v_copy(d, s + 1, c, 0).start()
        for d in range(2):
            n, m = len(over), (-s if d == 0 else s)
            v_over(n, m, False).start()
            over.append((n, m))
        if s == hx - 2:
            c_forward(1, 0)
    c_forward(1, 1)
    for d in range(2):
        v_copy(d, hx, d, 1).wait_recv()
    v_over(len(over), hx, False).start()
    over.append((len(over), hx))
    for n, m in over:
        v_over(n, m, True).wait_recv()
    h_copy.wait()

    tile = 128
    tiles = -(-rows // tile)
    for t in range(tiles):
        if t == tiles // 2:
            c_forward(2, 0)
        i0 = min(t * tile, rows - tile)
        lhs = hbuf[pl.ds(i0, tile), :, :].reshape(2 * tile, cols)
        part = lax.dot_general(lhs, vtall_ref[...], NT, preferred_element_type=F32)
        for n in range(vir // LANES):
            xs[n, pl.ds(2 * i0, 2 * tile), :] = part[:, n * LANES : (n + 1) * LANES]
    c_forward(2, 1)
    for n in range(vir // LANES):
        xs[n, pl.ds(2 * rows, 2 * (padded - rows)), :] = jnp.zeros((2 * (padded - rows), LANES), F32)
    for n in range(ncol):
        xo[n] = xs.at[n // 2][pl.ds(n % 2, padded, stride=2), :]

    base = ((0, half), (0, half - 1))

    def length(d, c):
        return half if d == c else half - 1

    def slot(d, c, s):
        return base[d][c] + s - 1

    def own(m, c):
        return xo[at_y(m), pl.ds(*chunks[c]), :]

    def r_copy(d, c, s):
        n = slot(d, c, s)
        size = pl.ds(0, chunks[c][1])
        src = rs0.at[d, c, size] if s == 1 else rsb.at[d, slot(d, c, s - 1), size]
        return remote(src, rsb.at[d, n, size], r_s.at[d, n], r_r.at[d, n], y_next[d])

    chains = ((0, 0), (1, 1), (0, 1), (1, 0))
    for d, c in chains:
        m = length(d, c)
        rs0[d, c, pl.ds(0, chunks[c][1]), :] = own(m if d == 0 else -m, c).astype(BF16)
        r_copy(d, c, 1).start()
    for s in range(1, half):
        for d, c in chains:
            if s < length(d, c):
                r_copy(d, c, s).wait_recv()
                m = length(d, c) - s
                at = (d, slot(d, c, s), pl.ds(0, chunks[c][1]))
                rsb[at] = (rsb[at].astype(F32) + own(m if d == 0 else -m, c)).astype(BF16)
                r_copy(d, c, s + 1).start()
        if s == half - 2:
            c_forward(half - 1, 0)
            c_forward(half - 1, 1)
    image = []
    for c in range(2):
        total = own(0, c)
        for d in range(2):
            r_copy(d, c, length(d, c)).wait_recv()
            at = (d, slot(d, c, length(d, c)), pl.ds(0, chunks[c][1]))
            total = total + rsb[at].astype(F32)
        image.append(total)
    image = jnp.concatenate(image, axis=0).T.astype(BF16)

    for d in range(2):
        c_arrived(d, half, d)

    for b in range(ncol):
        part = jnp.dot(image, cbuf[b], preferred_element_type=F32).astype(BF16)
        ct[0, b] = part[:, 0:LANES]
        ct[1, b] = part[:, LANES:]
    pair = remote(ct.at[1 - k], cx, d_s, d_r, partner)
    pair.start()
    pair.wait_recv()
    red[...] = (ct[k].astype(F32) + cx[...].astype(F32)).astype(BF16)

    def a_copy(j):
        to = at_x(j)
        return remote(red.at[to], xr.at[j - 1], a_s.at[j - 1], a_r.at[j - 1], {"row": 2 * to + k})

    def g_copy(j, back):
        part = rb.at[k, at_x(-j) if back else x]
        return remote(part, part, g_s.at[j - 1], g_r.at[j - 1], {"row": 2 * at_x(j) + k})

    far = sorted(range(1, nx), key=lambda j: -min(j, nx - j))
    for j in far:
        a_copy(j).start()
    total = red[x].astype(F32)
    for j in reversed(far):
        a_copy(j).wait_recv()
        total = total + xr[j - 1].astype(F32)
    rb[k, x] = (total / gap).astype(BF16)
    for j in far:
        g_copy(j, False).start()
    for j in reversed(far):
        g_copy(j, True).wait_recv()
    give = remote(rb.at[k], rb.at[k], e_s, e_r, partner)
    give.start()
    take = remote(rb.at[1 - k], rb.at[1 - k], e_s, e_r, partner)
    take.wait_recv()

    mixed = jnp.zeros((padded, LANES), F32)
    for b in range(ncol):
        resp = jnp.concatenate([rb[0, b], rb[1, b]], axis=1)
        mixed = mixed + lax.dot_general(cbuf[b], resp, NT, preferred_element_type=F32)
    mix_ref[y] = mixed.astype(BF16)
    m_send, m_arrived, m_drain = ring(mix_ref, m_s, m_r)
    for c in range(2):
        for d in range(2):
            m_send(d, 1, c)
    for s in range(1, half):
        for c in range(2):
            for d in range(2):
                m_arrived(d, s, c)
                if s + 1 < half or c == d:
                    m_send(d, s + 1, c)
    for d in range(2):
        m_arrived(d, half, d)

    for d in range(2):
        for s in range(1, hx + 1):
            for c in range(2) if s < hx else (d,):
                v_copy(d, s, c, 0).wait_send()
    for n, m in over:
        v_over(n, m, False).wait_send()
    c_drain()
    for d, c in chains:
        for s in range(1, length(d, c) + 1):
            r_copy(d, c, s).wait_send()
    pair.wait_send()
    for j in far:
        a_copy(j).wait_send()
        g_copy(j, False).wait_send()
    give.wait_send()
    m_drain()


def density_kernel(mix_ref, vt_ref, out_ref, lhs):
    count, tile = mix_ref.shape[0], mix_ref.shape[1]
    for n in range(count):
        lhs.at[n // 2][pl.ds(n % 2, tile, stride=2), :] = mix_ref[n].astype(F32)
    both = jnp.concatenate([lhs[n].astype(BF16) for n in range(count // 2)], axis=1)
    total = jnp.dot(both, vt_ref[...], preferred_element_type=F32)
    out_ref[...] = total.astype(BF16).reshape(out_ref.shape)


def per_device(nrow, ncol, perturbation, occ_coeffs, vir_coeffs, occ_energies, vir_energies):
    pert, rows, cols = perturbation.shape
    occ, vir = occ_energies.shape[0], vir_energies.shape[0]
    nocc, nx, half = occ_coeffs.shape[1], nrow // 2, ncol // 2
    padded = round_up(rows, 16)
    cut = round_up(padded // 2, 16)
    assert pert == 2 and pert * vir == ncol * LANES and nx == ncol and nocc <= 2 * LANES
    dma = pltpu.SemaphoreType.DMA
    ring = 2 * half - 1
    dims = (nrow, ncol, rows, cols, occ, vir)
    vmem = pl.BlockSpec(memory_space=pltpu.VMEM)
    mixed, vt_all = pl.pallas_call(
        functools.partial(exchange_kernel, dims),
        out_shape=(
            jax.ShapeDtypeStruct((ncol, padded, LANES), BF16),
            jax.ShapeDtypeStruct((vir, cols), BF16),
        ),
        in_specs=[pl.BlockSpec(memory_space=pl.ANY)] + [vmem] * 4,
        out_specs=(vmem, vmem),
        scratch_shapes=[
            pltpu.VMEM((rows, pert, cols), BF16),
            pltpu.VMEM((vir // LANES, 2 * padded, LANES), F32),
            pltpu.VMEM((ncol, padded, LANES), F32),
            pltpu.VMEM((ncol, padded, 2 * LANES), BF16),
            pltpu.VMEM((2, 2, cut, LANES), BF16),
            pltpu.VMEM((2, ring, cut, LANES), BF16),
            pltpu.VMEM((2, ncol, LANES, LANES), BF16),
            pltpu.VMEM((ncol, LANES, LANES), BF16),
            pltpu.VMEM((ncol, LANES, LANES), BF16),
            pltpu.VMEM((nx - 1, LANES, LANES), BF16),
            pltpu.VMEM((2, ncol, LANES, LANES), BF16),
            pltpu.VMEM((1, round_up(occ, LANES) + 2 * LANES), F32),
            dma,
            dma((2, ring)),
            dma((2, ring)),
            dma((nx,)),
            dma((nx,)),
            dma((2, ring)),
            dma((2, ring)),
            dma((2, ring)),
            dma((2, ring)),
            dma,
            dma,
            dma((nx - 1,)),
            dma((nx - 1,)),
            dma((nx - 1,)),
            dma((nx - 1,)),
            dma,
            dma,
            dma((2, ring)),
            dma((2, ring)),
        ],
        compiler_params=pltpu.CompilerParams(
            collective_id=0, has_side_effects=True, vmem_limit_bytes=56 * 2**20
        ),
        name="exchange",
    )(
        perturbation.transpose(1, 0, 2),
        vir_coeffs.T,
        occ_coeffs,
        occ_energies.reshape(1, occ),
        vir_energies.reshape(1, vir),
    )
    tile = 128
    density = pl.pallas_call(
        density_kernel,
        out_shape=jax.ShapeDtypeStruct((rows, pert, cols), BF16),
        grid=(-(-rows // tile),),
        in_specs=[
            pl.BlockSpec((ncol, tile, LANES), lambda i: (0, i, 0)),
            pl.BlockSpec((vir, cols), lambda i: (0, 0)),
        ],
        out_specs=pl.BlockSpec((tile, pert, cols), lambda i: (i, 0, 0)),
        scratch_shapes=[pltpu.VMEM((vir // LANES, pert * tile, LANES), F32)],
        compiler_params=pltpu.CompilerParams(vmem_limit_bytes=40 * 2**20),
        name="density",
    )(mixed, vt_all)
    return density.transpose(1, 0, 2)


def solution(mesh):
    spec = P("grp", "row", "col")
    return jax.shard_map(
        functools.partial(per_device, mesh.shape["row"], mesh.shape["col"]),
        mesh=mesh,
        in_specs=(spec, P("row", "col"), P("col", "row"), P(), P()),
        out_specs=spec,
        check_vma=False,
    )
```
